32 devices in a mesh: pipe: 4 (over z), row: 4 (over x, core), col: 2 (over y).
Axes of the slice: x: 2, y: 2, z: 4, core: 2. Of those that a mesh axis runs over, the one named last changes fastest.
Arguments:
- weights: bfloat16 [4, 4096, 14336], P('pipe', 'col', 'row'), may hold values from -0.09375 to 0.09375
- fwd_resid: bfloat16 [4, 128, 4096], P('pipe', None, 'col'), may hold values from -6 to 6
- fwd_hidden: bfloat16 [4, 128, 14336], P('pipe', None, 'row'), may hold values from -6 to 6
- bwd_resid: bfloat16 [4, 128, 4096], P('pipe', None, 'col'), may hold values from -6 to 6
- bwd_hidden: bfloat16 [4, 128, 14336], P('pipe', None, 'row'), may hold values from -6 to 6
- saved_pre: bfloat16 [4, 4, 128, 14336], P(None, 'pipe', None, 'row'), may hold values from -6 to 6
- pool_embed: bfloat16 [3, 128, 4096], P(None, None, 'col'), may hold values from -6 to 6
- pool_mask: int32 [3, 128], replicated, may hold values 0 or 1
- pool_stratum: int32 [3], replicated, may hold values from 0 to 7
- order: int32 [3], replicated, may hold values from 0 to 2, each once
- mask_vec: bfloat16 [4096], P('col'), may hold values from -6 to 6
- ratio_table: bfloat16 [8, 4096], P(None, 'col'), may hold values from -6 to 6
- cot_inject: bfloat16 [3, 128, 4096], P(None, None, 'col'), may hold values from -6 to 6
Outputs:
- out_resid: bfloat16 [2, 4, 128, 4096], P(None, 'pipe', None, 'col')
- out_hidden: bfloat16 [4, 128, 14336], P('pipe', 'col', 'row')
The draws below stay inside these ranges and needn't reach their ends.
Inputs may be any that keep to these rules, and one draw needn't show every extreme that they name: `order`: each waiting micro-batch enters exactly once.
All inputs are finite; a program needn't handle non-finite values.
Results may differ from the reference program's by a relative error of at most 0.025.
Values may be sent and summed in bfloat16 or wider, within the bound.
No kernel may reach another device: no remote copies, remote signals or barrier semaphores. Data moves between devices by JAX's collectives and lax.ppermute only.
A program may use at most 64 MiB of HBM per device.

```python
import jax
import jax.numpy as jnp
from jax import lax

D = 4096
F = 14336
MB_TOK = 128
STEPS = 4
STRATA = 8
POOL = 3
SECTIONS = 4
N_PIPE = 4
N_ROW = 4
N_COL = 2


def touch_ends(drawn, key, least, top_value):
    longest = drawn.shape.index(max(drawn.shape))
    spots = []
    for shift in (0, 1):
        where = [jax.random.randint(jax.random.fold_in(key, axis), (), 0, length) for axis, length in enumerate(drawn.shape)]
        where[longest] = (where[longest] + shift) % drawn.shape[longest]
        spots.append(tuple(where))
    return drawn.at[spots[0]].set(least).at[spots[1]].set(top_value)


def block_scale(rng, extent, pieces, smallest, largest):
    level = 1.0
    for axis_at, parts in pieces:
        steps = jax.random.uniform(jax.random.fold_in(jax.random.fold_in(rng, 6), axis_at), (parts,), jnp.float32, smallest / len(pieces), largest / len(pieces))
        level = level * jnp.repeat(jnp.exp(steps), extent[axis_at] // parts).reshape((-1,) + (1,) * (len(extent) - 1 - axis_at))
    return level


def noise(rng, extent, width, reach, split=(), kind=jnp.bfloat16):
    result = width * jax.random.normal(rng, extent, jnp.float32)
    if split:
        result = result * block_scale(rng, extent, split, -0.22, 0.18)
    return jnp.clip(result, -reach, reach).astype(kind)


def setup_inputs(seed: int = 0) -> dict:
    key_of = jax.random.split(jax.random.key(seed), 14)
    return {
        "weights": noise(key_of[0], (SECTIONS, D, F), D ** -0.5, 0.09375, ((0, 4), (1, 2), (2, 4))),
        "fwd_resid": noise(key_of[1], (SECTIONS, MB_TOK, D), 1.0, 6.0, ((0, 4), (2, 2))),
        "fwd_hidden": noise(key_of[2], (SECTIONS, MB_TOK, F), 1.0, 6.0, ((0, 4), (2, 4))),
        "bwd_resid": noise(key_of[3], (SECTIONS, MB_TOK, D), 1.0, 6.0, ((0, 4), (2, 2))),
        "bwd_hidden": noise(key_of[4], (SECTIONS, MB_TOK, F), 1.0, 6.0, ((0, 4), (2, 4))),
        "saved_pre": noise(key_of[5], (STEPS, SECTIONS, MB_TOK, F), 1.5, 6.0, ((1, 4), (3, 4))),
        "pool_embed": noise(key_of[6], (POOL, MB_TOK, D), 1.0, 6.0, ((2, 2),)),
        "pool_mask": touch_ends((jax.random.randint(key_of[7], (POOL, MB_TOK), 0, 2) < 1).astype(jnp.int32), jax.random.fold_in(key_of[7], 1), 0, 1),
        "pool_stratum": jax.random.randint(key_of[8], (POOL,), 0, STRATA).astype(jnp.int32),
        "order": jax.random.permutation(key_of[9], POOL).astype(jnp.int32),
        "mask_vec": noise(key_of[10], (D,), 1.0, 6.0, ((0, 2),)),
        "ratio_table": noise(key_of[11], (STRATA, D), 1.0, 6.0, ((1, 2),)),
        "cot_inject": noise(key_of[12], (POOL, MB_TOK, D), 1.0, 6.0, ((2, 2),)),
    }


def silu_grad(preact):
    sigma = jax.nn.sigmoid(preact)
    return sigma * (1.0 + preact * (1.0 - sigma))

def sum_features(operand, weight):
    block_width = D // N_COL

    def add_block(block, running):
        offset = (block * block_width).astype(jnp.int32)
        product = jnp.dot(lax.dynamic_slice_in_dim(operand, offset, block_width, 1), lax.dynamic_slice_in_dim(weight, offset, block_width, 0), preferred_element_type=jnp.float32)
        rounded = lax.optimization_barrier(product.astype(jnp.bfloat16))
        return running + rounded.astype(jnp.float32)
    return lax.fori_loop(0, N_COL, add_block, jnp.zeros((operand.shape[0], weight.shape[1]), jnp.float32))

def sum_hidden(operand, weight):
    block_width = F // N_ROW

    def add_block(block, running):
        offset = (block * block_width).astype(jnp.int32)
        product = lax.dot_general(lax.dynamic_slice_in_dim(operand, offset, block_width, 1), lax.dynamic_slice_in_dim(weight, offset, block_width, 1), (((1,), (1,)), ((), ())), preferred_element_type=jnp.float32)
        rounded = lax.optimization_barrier(product.astype(jnp.bfloat16))
        return running + rounded.astype(jnp.float32)
    return lax.fori_loop(0, N_ROW, add_block, jnp.zeros((operand.shape[0], weight.shape[0]), jnp.float32))

def section_update(inputs):
    section, weight, fwd_res, bwd_res, fwd_hid, bwd_hid, saved = inputs
    is_even = section % 2 == 0
    operand = jnp.where(is_even, fwd_res, bwd_res)
    preact = sum_features(operand, weight)
    hid_out = jnp.where(is_even, jax.nn.silu(preact), preact).astype(jnp.bfloat16)
    hid_grad = (bwd_hid.astype(jnp.float32) * silu_grad(saved.astype(jnp.float32))).astype(jnp.bfloat16)
    hid_operand = jnp.where(is_even, hid_grad, fwd_hid)
    residual = jnp.where(is_even, bwd_res, fwd_res)
    updated = (residual.astype(jnp.float32) + sum_hidden(hid_operand, weight)).astype(jnp.bfloat16)
    fwd_out = jnp.where(is_even, fwd_res, updated)
    bwd_out = jnp.where(is_even, updated, bwd_res)
    return (fwd_out, bwd_out, hid_out)

def inject(step_idx, pool_embed, pool_mask, pool_stratum, order, mask_vec, ratio_table):
    chosen = order[step_idx - 1]
    embedded = pool_embed[chosen]
    masked = pool_mask[chosen]
    stratum = pool_stratum[chosen]
    onehot = (jnp.arange(ratio_table.shape[0], dtype=jnp.int32) == stratum).astype(jnp.bfloat16)
    condition = jnp.dot(onehot, ratio_table, preferred_element_type=jnp.float32)
    chosen_rows = jnp.where(masked[:, None] == 1, mask_vec[None, :].astype(jnp.float32), embedded.astype(jnp.float32))
    return (chosen_rows + condition[None, :]).astype(jnp.bfloat16)

def reference(weights, fwd_resid, fwd_hidden, bwd_resid, bwd_hidden, saved_pre, pool_embed, pool_mask, pool_stratum, order, mask_vec, ratio_table, cot_inject):
    section_ids = jnp.arange(N_PIPE, dtype=jnp.int32)
    fwd_res, bwd_res, fwd_hid, bwd_hid = (fwd_resid, bwd_resid, fwd_hidden, bwd_hidden)
    fwd_out, bwd_out, hid_out = (fwd_res, bwd_res, fwd_hid)
    for step_idx in range(STEPS):
        if step_idx > 0:
            incoming = inject(step_idx, pool_embed, pool_mask, pool_stratum, order, mask_vec, ratio_table)
            fwd_res = jnp.concatenate([incoming[None], fwd_out[:-1]], 0)
            fwd_hid = jnp.concatenate([jnp.zeros_like(hid_out[:1]), hid_out[:-1]], 0)
            bwd_res = jnp.concatenate([bwd_out[1:], cot_inject[step_idx - 1][None]], 0)
            bwd_hid = jnp.concatenate([hid_out[1:], jnp.zeros_like(hid_out[:1])], 0)
        fwd_out, bwd_out, hid_out = lax.map(section_update, (section_ids, weights, fwd_res, bwd_res, fwd_hid, bwd_hid, saved_pre[step_idx]))
    return (jnp.stack([fwd_out, bwd_out]), hid_out)
```

```python
import functools

import jax
import jax.numpy as jnp
from jax import lax
from jax.experimental import pallas as pl
from jax.experimental.pallas import tpu as pltpu
from jax.sharding import PartitionSpec as P

STEPS = 4


def tile_of(length, width, budget):
    best = 128
    for tile in range(128, length + 1, 128):
        if length % tile == 0 and tile * width * 2 <= budget:
            best = tile
    return best


def up_kernel(info, own, other, weight, keep, send, operand):
    half = own.shape[0]

    @pl.when(pl.program_id(0) == 0)
    def _():
        side = info[0]
        operand[pl.ds(pl.multiple_of(side * half, half), half), :] = own[...]
        operand[pl.ds(pl.multiple_of((1 - side) * half, half), half), :] = other[...]

    product = jnp.dot(operand[...], weight[...], preferred_element_type=jnp.float32)
    keep[...] = product[:half].astype(keep.dtype)
    send[...] = product[half:].astype(send.dtype)


def up_product(info, own, other, weight):
    half, depth = own.shape
    width = weight.shape[1]
    tile = tile_of(width, depth, 2 * 1024 * 1024)
    whole = pl.BlockSpec((half, depth), lambda i, s: (0, 0))
    out = pl.BlockSpec((half, tile), lambda i, s: (0, i))
    shape = jax.ShapeDtypeStruct((half, width), jnp.bfloat16)
    return pl.pallas_call(
        up_kernel,
        grid_spec=pltpu.PrefetchScalarGridSpec(
            num_scalar_prefetch=1,
            grid=(width // tile,),
            in_specs=[whole, whole, pl.BlockSpec((depth, tile), lambda i, s: (0, i))],
            out_specs=[out, out],
            scratch_shapes=[pltpu.VMEM((2 * half, depth), jnp.bfloat16)],
        ),
        out_shape=[shape, shape],
        compiler_params=pltpu.CompilerParams(vmem_limit_bytes=32 * 1024 * 1024),
        cost_estimate=pl.CostEstimate(
            flops=4 * half * depth * width,
            bytes_accessed=2 * depth * width,
            transcendentals=0,
        ),
        name="up_product",
    )(info, own, other, weight)


def down_kernel(blocks, info, own, other, saved, weight, keep, send, operand):
    half = own.shape[0]
    rows = half * 2 // blocks

    @pl.when(pl.program_id(0) == 0)
    def _():
        @pl.when(info[1] == 1)
        def _():
            for block in range(blocks):
                source = own if block < blocks // 2 else other
                at = block * rows % half
                row = pl.multiple_of((block ^ info[2]) * rows, rows)
                preact = saved[0, 0, pl.ds(row, rows), :].astype(jnp.float32)
                sigma = 1.0 / (1.0 + jnp.exp(-preact))
                factor = sigma * (1.0 + preact * (1.0 - sigma))
                hidden = source[at : at + rows, :].astype(jnp.float32)
                operand[block * rows : (block + 1) * rows, :] = (hidden * factor).astype(
                    operand.dtype
                )

        @pl.when(info[1] == 0)
        def _():
            operand[:half, :] = own[...]
            operand[half:, :] = other[...]

    product = lax.dot_general(
        operand[...], weight[...], (((1,), (1,)), ((), ())), preferred_element_type=jnp.float32
    ).astype(jnp.bfloat16)
    upper = info[0] == 1
    keep[...] = jnp.where(upper, product[half:], product[:half])
    send[...] = jnp.where(upper, product[:half], product[half:])


def down_product(step_idx, blocks, info, own, other, saved, weight):
    half, width = own.shape
    depth = weight.shape[0]
    tile = tile_of(depth, width, 2 * 1024 * 1024)
    whole = pl.BlockSpec((half, width), lambda i, s: (0, 0))
    out = pl.BlockSpec((half, tile), lambda i, s: (0, i))
    shape = jax.ShapeDtypeStruct((half, depth), jnp.bfloat16)
    return pl.pallas_call(
        functools.partial(down_kernel, blocks),
        grid_spec=pltpu.PrefetchScalarGridSpec(
            num_scalar_prefetch=1,
            grid=(depth // tile,),
            in_specs=[
                whole,
                whole,
                pl.BlockSpec((1, 1, 2 * half, width), lambda i, s: (step_idx, 0, 0, 0)),
                pl.BlockSpec((tile, width), lambda i, s: (i, 0)),
            ],
            out_specs=[out, out],
            scratch_shapes=[pltpu.VMEM((2 * half, width), jnp.bfloat16)],
        ),
        out_shape=[shape, shape],
        compiler_params=pltpu.CompilerParams(vmem_limit_bytes=32 * 1024 * 1024),
        cost_estimate=pl.CostEstimate(
            flops=4 * half * depth * width,
            bytes_accessed=2 * depth * width,
            transcendentals=0,
        ),
        name="down_product",
    )(info, own, other, saved, weight)


def exchange(value, axis, mask):
    pairs = [(source, source ^ mask) for source in range(lax.axis_size(axis))]
    return lax.ppermute(value, axis, pairs)


def bits_of(axis):
    size = lax.axis_size(axis)
    bits = size.bit_length() - 1
    if 1 << bits != size:
        raise ValueError(axis)
    return bits


def inject(step_idx, row, rows, pool_embed, pool_mask, pool_stratum, order, mask_vec, ratio_table):
    chosen = order[step_idx - 1]
    embedded = lax.dynamic_slice(
        pool_embed, (chosen, row, 0), (1, rows, pool_embed.shape[2])
    )[0]
    masked = lax.dynamic_slice(pool_mask, (chosen, row), (1, rows))[0]
    condition = lax.dynamic_slice_in_dim(ratio_table, pool_stratum[chosen], 1, 0)
    chosen_rows = jnp.where(
        masked[:, None] == 1, mask_vec[None, :].astype(jnp.float32), embedded.astype(jnp.float32)
    )
    return (chosen_rows + condition.astype(jnp.float32)).astype(jnp.bfloat16)


def shards(
    weights,
    fwd_resid,
    fwd_hidden,
    bwd_resid,
    bwd_hidden,
    saved_pre,
    pool_embed,
    pool_mask,
    pool_stratum,
    order,
    mask_vec,
    ratio_table,
    cot_inject,
):
    weight = weights[0]
    position = lax.axis_index("pipe")
    sections = lax.axis_size("pipe")
    is_even = position % 2 == 0
    col = lax.axis_index("col")
    row = lax.axis_index("row")
    col_size = lax.axis_size("col")
    col_bits = bits_of("col")
    row_bits = bits_of("row")
    tokens = fwd_resid.shape[1]
    half = tokens // 2
    block = tokens // col_size
    core = row % 2
    even_int = is_even.astype(jnp.int32)
    up_info = core[None].astype(jnp.int32)
    down_info = jnp.stack([core, even_int, col]).astype(jnp.int32)

    def local_rows(value):
        parts = [
            lax.dynamic_slice_in_dim(value, (at ^ col) * block, block, 0)
            for at in range(col_size)
        ]
        return jnp.concatenate(parts, 0)

    share = tokens
    first = jnp.int32(0)
    for bit in range(row_bits):
        share //= 2
        first = first + ((row >> bit) & 1) * share
    row_block = first // block
    within = first % block

    def own_tokens():
        if share <= block:
            return [((row_block ^ col) * block + within, share)]
        count = share // block
        return [(((row_block + at) ^ col) * block, block) for at in range(count)]

    def own_share(value):
        parts = [lax.dynamic_slice_in_dim(value, at, n, 0) for at, n in own_tokens()]
        return parts[0] if len(parts) == 1 else jnp.concatenate(parts, 0)

    def joined(mine, theirs, bit):
        upper = ((row >> bit) & 1) == 1
        return jnp.where(
            upper, jnp.concatenate([theirs, mine], 0), jnp.concatenate([mine, theirs], 0)
        )

    def scatter_rows(keep, send):
        total = keep.astype(jnp.float32) + exchange(send, "row", 1).astype(jnp.float32)
        for bit in range(1, row_bits):
            part = total.shape[0] // 2
            upper = ((row >> bit) & 1) == 1
            mine = jnp.where(upper, total[part:], total[:part])
            theirs = jnp.where(upper, total[:part], total[part:]).astype(jnp.bfloat16)
            total = mine + exchange(theirs, "row", 1 << bit).astype(jnp.float32)
        return total

    def gather_rows(value):
        for bit in reversed(range(1, row_bits)):
            value = joined(value, exchange(value, "row", 1 << bit), bit)
        return value, exchange(value, "row", 1)

    def scatter_cols(keep, send):
        total = keep.astype(jnp.float32)
        for bit in reversed(range(col_bits)):
            received = exchange(send, "col", 1 << bit).astype(jnp.float32)
            total = total + received
            if bit:
                part = total.shape[0] // 2
                send = total[part:].astype(jnp.bfloat16)
                total = total[:part]
        return total

    def gather_cols(value):
        for bit in range(col_bits - 1):
            value = jnp.concatenate([value, exchange(value, "col", 1 << bit)], 0)
        return value, exchange(value, "col", 1 << (col_bits - 1))

    pair_up = [(at, at + 1) for at in range(1, sections - 1, 2)]
    cross = pair_up + [(to, at) for at, to in pair_up]
    pool = (pool_embed, pool_mask, pool_stratum, order, mask_vec, ratio_table)

    operand = local_rows(jnp.where(is_even, fwd_resid[0], bwd_resid[0]))
    operand_parts = (operand[:half], operand[half:])
    operand_share = own_share(jnp.where(is_even, fwd_resid[0], bwd_resid[0]))
    residual = own_share(jnp.where(is_even, bwd_resid[0], fwd_resid[0]))
    hidden = local_rows(jnp.where(is_even, bwd_hidden[0], fwd_hidden[0]))
    hidden_parts = (hidden[:half], hidden[half:])
    side = jnp.zeros((1,), jnp.int32)
    for step_idx in range(STEPS):
        keep, send = up_product(side, *operand_parts, weight)
        side = up_info
        preact = scatter_cols(keep, send)
        hid_share = jnp.where(is_even, jax.nn.silu(preact), preact).astype(jnp.bfloat16)
        keep, send = down_product(
            step_idx, col_size, down_info, *hidden_parts, saved_pre, weight
        )
        blended = scatter_rows(keep, send)
        updated = (residual.astype(jnp.float32) + blended).astype(jnp.bfloat16)
        if step_idx + 1 < STEPS:
            hidden_parts = gather_cols(exchange(hid_share, "pipe", 1))
            residual = exchange(operand_share, "pipe", 1)
            incoming = jnp.concatenate(
                [inject(step_idx + 1, at, n, *pool) for at, n in own_tokens()], 0
            )
            entering = jnp.where(position == 0, incoming, own_share(cot_inject[step_idx]))
            is_end = (position == 0) | (position == sections - 1)
            operand_share = jnp.where(is_end, entering, lax.ppermute(updated, "pipe", cross))
            operand_parts = gather_rows(operand_share)
    last_operand = local_rows(joined(*operand_parts, 0))
    last_updated = local_rows(joined(*gather_rows(updated), 0))
    out_resid = jnp.stack(
        [
            jnp.where(is_even, last_operand, last_updated),
            jnp.where(is_even, last_updated, last_operand),
        ]
    )[:, None]
    return (out_resid, hid_share[None])


def solution(mesh):
    return jax.shard_map(
        shards,
        mesh=mesh,
        in_specs=(
            P("pipe", "col", "row"),
            P("pipe", None, "col"),
            P("pipe", None, "row"),
            P("pipe", None, "col"),
            P("pipe", None, "row"),
            P(None, "pipe", None, "row"),
            P(None, None, "col"),
            P(),
            P(),
            P(),
            P("col"),
            P(None, "col"),
            P(None, None, "col"),
        ),
        out_specs=(P(None, "pipe", None, "col"), P("pipe", "col", "row")),
        check_vma=False,
    )
```

```python
import functools

import jax
import jax.numpy as jnp
from jax import lax
from jax.experimental import pallas as pl
from jax.experimental.pallas import tpu as pltpu
from jax.sharding import PartitionSpec as P

STEPS = 4
CHUNKS = 2
MIB = 1024 * 1024

VMEM = pl.BlockSpec(memory_space=pltpu.VMEM)
SMEM = pl.BlockSpec(memory_space=pltpu.SMEM)
HBM = pl.BlockSpec(memory_space=pltpu.HBM)
BF16 = jnp.bfloat16
F32 = jnp.float32
PIPE, ROW, COL = "pipe", "row", "col"


def tile_of(length, limit):
    return max(tile for tile in range(128, limit + 1, 128) if length % tile == 0)


def call(kernel, name, in_specs, outs, scratch=(), grant=4 * MIB, flops=0, nbytes=0):
    return pl.pallas_call(
        kernel,
        in_specs=in_specs,
        out_specs=[pl.BlockSpec(memory_space=space) for _, _, space in outs],
        out_shape=[space(shape, kind) for shape, kind, space in outs],
        scratch_shapes=list(scratch),
        compiler_params=pltpu.CompilerParams(vmem_limit_bytes=grant),
        cost_estimate=pl.CostEstimate(flops=flops, bytes_accessed=nbytes, transcendentals=0),
        name=name,
    )


def place(axis):
    return lax.axis_index(axis).astype(jnp.int32)


def token_row(local, block):
    return pl.multiple_of((local // block ^ place(COL)) * block + local % block, 16)


def share_start(tokens, bits):
    start, share = jnp.int32(0), tokens
    for bit in range(bits):
        share //= 2
        start = start + (place(ROW) >> bit & 1) * share
    return start, share


def is_even():
    return place(PIPE) % 2 == 0


def by_parity(even, odd, make):
    @pl.when(is_even())
    def _():
        make(even).start()

    @pl.when(jnp.logical_not(is_even()))
    def _():
        make(odd).start()

    return make(even)


def multiply(operand, weight, keep, send, at, tile):
    half = keep.shape[0]
    columns = slice(at, at + tile)
    product = jnp.dot(operand[...], weight[:, columns], preferred_element_type=F32)
    keep[:, columns] = product[:half].astype(BF16)
    send[:, columns] = product[half:].astype(BF16)


def load_kernel(chunk, block, even, odd, source, *refs):
    if chunk == 0:
        weight, keep, send, operand, tile_sems, row_sems = refs
    else:
        operand, weight, keep, send, tile_sems = refs
    width = weight.shape[1]
    tile = width // tile_sems.shape[0]
    copies = []
    if chunk == 0:
        for at in range(0, operand.shape[0], block):
            rows = pl.ds(token_row(at, block), block)
            copies.append(
                by_parity(
                    even,
                    odd,
                    lambda ref, rows=rows, at=at: pltpu.make_async_copy(
                        ref.at[0, rows, :], operand.at[at : at + block], row_sems.at[at // block]
                    ),
                )
            )
    loads = []
    for at in range(0, width, tile):
        columns = slice(chunk * width + at, chunk * width + at + tile)
        loads.append(
            pltpu.make_async_copy(
                source.at[0, :, columns], weight.at[:, at : at + tile], tile_sems.at[at // tile]
            )
        )
        loads[-1].start()
    for copy in copies:
        copy.wait()
    for index, load in enumerate(loads):
        load.wait()
        multiply(operand, weight, keep, send, index * tile, tile)


def up_kernel(tile, operand, weight, keep, send):
    for at in range(0, weight.shape[1], tile):
        multiply(operand, weight, keep, send, at, tile)


def factor_kernel(step_idx, chunk, block, saved, factor, stored, sems):
    tokens, width = factor.shape
    even = is_even()

    @pl.when(even)
    def _():
        copies = []
        for at in range(0, tokens, block):
            rows = pl.ds(token_row(at, block), block)
            copies.append(
                pltpu.make_async_copy(
                    saved.at[step_idx, 0, rows, chunk * width : (chunk + 1) * width],
                    stored.at[at : at + block],
                    sems.at[at // block],
                )
            )
            copies[-1].start()
        for copy in copies:
            copy.wait()

        def body(index, carry):
            rows = pl.ds(pl.multiple_of(index * 16, 16), 16)
            preact = stored[rows, :].astype(F32)
            sigma = 0.5 * jnp.tanh(0.5 * preact) + 0.5
            factor[rows, :] = sigma * (1.0 + preact * (1.0 - sigma))
            return carry

        lax.fori_loop(0, tokens // 16, body, 0)

    @pl.when(jnp.logical_not(even))
    def _():
        factor[...] = jnp.ones_like(factor)


def down_kernel(tile, first, last, flip, own, other, factor, weight, *refs):
    refs = list(refs)
    total = None if first else refs.pop(0)
    operand = refs.pop()
    flipped = refs.pop() if flip else weight
    half = own.shape[0]
    operand[:half] = (own[...].astype(F32) * factor[:half]).astype(BF16)
    operand[half:] = (other[...].astype(F32) * factor[half:]).astype(BF16)
    upper = (place(ROW) & 1) == 1
    for at in range(0, flipped.shape[1], tile):
        columns = slice(at, at + tile)
        if flip:
            turned = weight[columns, :].T
            flipped[:, columns] = turned
        else:
            turned = weight[:, columns]
        product = jnp.dot(operand[...], turned, preferred_element_type=F32)
        if not first:
            product = product + total[:, columns]
        if last:
            keep, send = refs
            low, high = product[:half].astype(BF16), product[half:].astype(BF16)
            keep[:, columns] = jnp.where(upper, high, low)
            send[:, columns] = jnp.where(upper, low, high)
        else:
            refs[0][:, columns] = product


def hidden_kernel(block, even, odd, *refs):
    *outs, sems = refs
    half, width = outs[0].shape
    copies = []
    for at in range(0, 2 * half, block):
        rows = pl.ds(token_row(at, block), block)
        for chunk in range(CHUNKS):
            target = outs[2 * chunk + at // half]
            index = at // block * CHUNKS + chunk
            copies.append(
                by_parity(
                    even,
                    odd,
                    lambda ref, rows=rows, at=at, chunk=chunk, target=target, index=index: (
                        pltpu.make_async_copy(
                            ref.at[0, rows, chunk * width : (chunk + 1) * width],
                            target.at[at % half : at % half + block],
                            sems.at[index],
                        )
                    ),
                )
            )
    for copy in copies:
        copy.wait()


def share_kernel(block, bits, fwd, bwd, operand_share, residual, sems):
    start, share = share_start(fwd.shape[1], bits)
    pieces = max(1, share // block)
    size = share // pieces
    copies = []
    for piece in range(pieces):
        rows = pl.ds(token_row(start + piece * size, block), size)
        target = slice(piece * size, (piece + 1) * size)
        for index, (even, odd, out) in enumerate(
            ((fwd, bwd, operand_share), (bwd, fwd, residual))
        ):
            copies.append(
                by_parity(
                    even,
                    odd,
                    lambda ref, rows=rows, target=target, out=out, at=piece * 2 + index: (
                        pltpu.make_async_copy(ref.at[0, rows, :], out.at[target], sems.at[at])
                    ),
                )
            )
    for copy in copies:
        copy.wait()


def entering_kernel(
    block, bits, sections, order, stratum, embed, mask, vector, table, cot, *refs
):
    *outs, stored, sem = refs
    tokens = mask.shape[1]
    start, share = share_start(tokens, bits)
    pieces = max(1, share // block)
    size = share // pieces
    for step_idx, out in enumerate(outs):
        for piece in range(pieces):
            row = token_row(start + piece * size, block)
            target = slice(piece * size, (piece + 1) * size)

            @pl.when(place(PIPE) == 0)
            def _():
                chosen = order[step_idx]
                copy = pltpu.make_async_copy(embed.at[chosen, pl.ds(row, size), :], stored, sem)
                copy.start()
                copy.wait()
                masked = mask[chosen, pl.ds(row, size), :]
                rows = jnp.where(
                    masked[:, :1] == 1, vector[...].astype(F32), stored[...].astype(F32)
                )
                condition = table[pl.ds(stratum[chosen], 1), :]
                out[target, :] = (rows + condition).astype(BF16)

            @pl.when(place(PIPE) == sections - 1)
            def _():
                copy = pltpu.make_async_copy(
                    cot.at[step_idx, pl.ds(row, size), :], out.at[target], sem
                )
                copy.start()
                copy.wait()


def act_kernel(keep, received, out):
    def body(index, carry):
        rows = pl.ds(pl.multiple_of(index * 16, 16), 16)
        preact = keep[rows, :].astype(F32) + received[rows, :].astype(F32)
        active = preact * (0.5 * jnp.tanh(0.5 * preact) + 0.5)
        out[rows, :] = jnp.where(is_even(), active, preact).astype(BF16)
        return carry

    lax.fori_loop(0, keep.shape[0] // 16, body, 0)


def split_kernel(bit, keep, received, mine, theirs):
    part = mine.shape[0]
    upper = place(ROW) >> bit & 1
    rows = pl.ds(pl.multiple_of(upper * part, part), part)
    mine[...] = keep[rows, :].astype(F32) + received[rows, :].astype(F32)
    rows = pl.ds(pl.multiple_of((1 - upper) * part, part), part)
    theirs[...] = (keep[rows, :].astype(F32) + received[rows, :].astype(F32)).astype(BF16)


def enter_kernel(sections, received, entering, out):
    end = (place(PIPE) == 0) | (place(PIPE) == sections - 1)

    @pl.when(end)
    def _():
        out[...] = entering[...]

    @pl.when(jnp.logical_not(end))
    def _():
        out[...] = received[...]


def join_kernel(bit, mine, theirs, out):
    part = mine.shape[0]
    upper = place(ROW) >> bit & 1
    out[pl.ds(pl.multiple_of(upper * part, part), part), :] = mine[...]
    out[pl.ds(pl.multiple_of((1 - upper) * part, part), part), :] = theirs[...]


def output_kernel(block, operand, mine, theirs, out, sems):
    tokens = operand.shape[0]
    half = tokens // 2
    even = is_even().astype(jnp.int32)
    copies = []
    for at in range(0, tokens, block):
        rows = pl.ds(token_row(at, block), block)
        copies.append(
            pltpu.make_async_copy(
                operand.at[at : at + block], out.at[1 - even, 0, rows, :], sems.at[len(copies)]
            )
        )
    upper = place(ROW) & 1
    for source, side in ((mine, upper), (theirs, 1 - upper)):
        for at in range(0, half, block):
            rows = pl.ds(token_row(side * half + at, block), block)
            copies.append(
                pltpu.make_async_copy(
                    source.at[at : at + block], out.at[even, 0, rows, :], sems.at[len(copies)]
                )
            )
    for copy in copies:
        copy.start()
    for copy in copies:
        copy.wait()


def exchange(value, axis, mask):
    pairs = [(source, source ^ mask) for source in range(lax.axis_size(axis))]
    return lax.ppermute(value, axis, pairs)


def bits_of(axis):
    size = lax.axis_size(axis)
    bits = size.bit_length() - 1
    if 1 << bits != size:
        raise ValueError(axis)
    return bits


def shards(
    weights,
    fwd_resid,
    fwd_hidden,
    bwd_resid,
    bwd_hidden,
    saved_pre,
    pool_embed,
    pool_mask,
    pool_stratum,
    order,
    mask_vec,
    ratio_table,
    cot_inject,
):
    weights, fwd_resid, fwd_hidden, bwd_resid, bwd_hidden, saved_pre, pool_embed, cot_inject = (
        pltpu.with_memory_space_constraint(value, pltpu.HBM)
        for value in (
            weights,
            fwd_resid,
            fwd_hidden,
            bwd_resid,
            bwd_hidden,
            saved_pre,
            pool_embed,
            cot_inject,
        )
    )
    sections = lax.axis_size("pipe")
    col_size = lax.axis_size("col")
    col_bits = bits_of("col")
    row_bits = bits_of("row")
    _, depth, hidden_width = weights.shape
    tokens = fwd_resid.shape[1]
    half = tokens // 2
    share = tokens >> row_bits
    block = tokens // col_size
    width = hidden_width // CHUNKS
    up_tile = tile_of(width, 256)
    down_tile = tile_of(depth, 256)
    product_cost = dict(flops=2 * tokens * depth * width, nbytes=2 * depth * width)
    dma = pltpu.SemaphoreType.DMA
    halves = [((half, width), BF16, pltpu.VMEM)] * 2

    def load(chunk, operand):
        outs = [((depth, width), BF16, pltpu.VMEM)] + halves
        scratch = [dma((width // up_tile,))]
        if chunk == 0:
            outs = outs + [((tokens, depth), BF16, pltpu.VMEM)]
            scratch = scratch + [dma((col_size,))]
        rest = [] if operand is None else [operand]
        return call(
            functools.partial(load_kernel, chunk, block),
            f"load_{chunk}",
            [HBM, HBM, HBM] + [VMEM] * len(rest),
            outs,
            scratch,
            **product_cost,
        )(fwd_resid, bwd_resid, weights, *rest)

    def up(operand, weight):
        return call(
            functools.partial(up_kernel, up_tile), "up", [VMEM] * 2, halves, **product_cost
        )(operand, weight)

    def factor(step_idx, chunk):
        return call(
            functools.partial(factor_kernel, step_idx, chunk, block),
            f"factor_{step_idx}_{chunk}",
            [HBM],
            [((tokens, width), F32, pltpu.VMEM)],
            [pltpu.VMEM((tokens, width), BF16), dma((col_size,))],
            flops=40 * tokens * width,
            nbytes=2 * tokens * width,
        )(saved_pre)[0]

    def down(chunk, own, other, factors, weight, total, flip):
        first, last = chunk == 0, chunk == CHUNKS - 1
        outs = [((half, depth), BF16, pltpu.VMEM)] * 2
        outs = outs if last else [((tokens, depth), F32, pltpu.VMEM)]
        rest = [] if first else [total]
        return call(
            functools.partial(down_kernel, down_tile, first, last, flip),
            f"flip_{chunk}" if flip else f"down_{chunk}",
            [VMEM] * (4 + len(rest)),
            outs + [((width, depth), BF16, pltpu.VMEM)] * flip,
            [pltpu.VMEM((tokens, width), BF16)],
            **product_cost,
        )(own, other, factors, weight, *rest)

    def small(kernel, name, outs, *operands):
        work = operands[0].size
        return call(
            kernel, name, [VMEM] * len(operands), outs, flops=100 * work, nbytes=4 * work
        )(*operands)

    def joined(mine, theirs, bit):
        outs = [((2 * mine.shape[0], depth), BF16, pltpu.VMEM)]
        return small(functools.partial(join_kernel, bit), f"join_{bit}", outs, mine, theirs)[0]

    def scatter_rows(keep, send):
        received = exchange(send, "row", 1)
        for bit in range(1, row_bits):
            part = keep.shape[0] // 2
            outs = [((part, depth), F32, pltpu.VMEM), ((part, depth), BF16, pltpu.VMEM)]
            keep, send = small(
                functools.partial(split_kernel, bit), f"split_{bit}", outs, keep, received
            )
            received = exchange(send, "row", 1 << bit)
        return keep, received

    def gather_rows(value):
        for bit in reversed(range(1, row_bits)):
            value = joined(value, exchange(value, "row", 1 << bit), bit)
        return value, exchange(value, "row", 1)

    def scatter_cols(keep, send):
        received = exchange(send, "col", 1 << (col_bits - 1))
        for bit in reversed(range(col_bits - 1)):
            total = keep.astype(F32) + received.astype(F32)
            part = total.shape[0] // 2
            keep = total[:part]
            received = exchange(total[part:].astype(BF16), "col", 1 << bit)
        return keep, received

    def gather_cols(value):
        for bit in range(col_bits - 1):
            value = jnp.concatenate([value, exchange(value, "col", 1 << bit)], 0)
        return value, exchange(value, "col", 1 << (col_bits - 1))

    def activated(keep, received):
        return small(act_kernel, "act", [(keep.shape, BF16, pltpu.VMEM)], keep, received)[0]

    pair_up = [(at, at + 1) for at in range(1, sections - 1, 2)]
    cross = pair_up + [(to, at) for at, to in pair_up]
    share_out = ((share, depth), BF16, pltpu.VMEM)
    pieces = max(1, share // block)

    weight, flipped, operand, products = [], [], None, []
    for chunk in range(CHUNKS):
        loaded, keep, send, *rest = load(chunk, operand)
        operand = rest[0] if rest else operand
        weight.append(loaded)
        products.append((keep, send))
    hidden = call(
        functools.partial(hidden_kernel, block),
        "hidden",
        [HBM, HBM],
        halves * CHUNKS,
        [dma((col_size * CHUNKS,))],
        nbytes=2 * tokens * hidden_width,
    )(bwd_hidden, fwd_hidden)
    hidden = [tuple(hidden[2 * chunk : 2 * chunk + 2]) for chunk in range(CHUNKS)]
    operand_share, residual = call(
        functools.partial(share_kernel, block, row_bits),
        "share",
        [HBM, HBM],
        [share_out] * 2,
        [dma((2 * pieces,))],
        nbytes=4 * share * depth,
    )(fwd_resid, bwd_resid)
    mask = jnp.broadcast_to(pool_mask[:, :, None], pool_mask.shape + (128,))
    entering = call(
        functools.partial(entering_kernel, block, row_bits, sections),
        "entering",
        [SMEM, SMEM, HBM, VMEM, VMEM, VMEM, HBM],
        [share_out] * (STEPS - 1),
        [pltpu.VMEM((share // pieces, depth), BF16), dma],
        nbytes=6 * share * depth,
    )(order, pool_stratum, pool_embed, mask, mask_vec[None], ratio_table.astype(F32), cot_inject)

    for step_idx in range(STEPS):
        if step_idx:
            products = [up(operand, weight[chunk]) for chunk in range(CHUNKS)]
        hid_share = [activated(*scatter_cols(*pair)) for pair in products]
        total = None
        for chunk in range(CHUNKS):
            flip = step_idx == 0
            total, *rest = down(
                chunk,
                *hidden[chunk],
                factor(step_idx, chunk),
                weight[chunk] if flip else flipped[chunk],
                total,
                flip,
            )
            if flip:
                flipped.append(rest.pop())
        blended = scatter_rows(total, *rest)
        updated = sum(value.astype(F32) for value in (*blended, residual)).astype(BF16)
        if step_idx + 1 < STEPS:
            hidden = [gather_cols(exchange(value, "pipe", 1)) for value in hid_share]
            residual = exchange(operand_share, "pipe", 1)
            operand_share = small(
                functools.partial(enter_kernel, sections),
                "enter",
                [share_out],
                lax.ppermute(updated, "pipe", cross),
                entering[step_idx],
            )[0]
            operand = joined(*gather_rows(operand_share), 0)
    out_resid = call(
        functools.partial(output_kernel, block),
        "output",
        [VMEM, VMEM, VMEM],
        [((2, 1, tokens, depth), BF16, pltpu.HBM)],
        [dma((2 * col_size,))],
        nbytes=4 * tokens * depth,
    )(operand, *gather_rows(updated))[0]
    return (out_resid, jnp.concatenate(hid_share, 1)[None])


def solution(mesh):
    return jax.shard_map(
        shards,
        mesh=mesh,
        in_specs=(
            P("pipe", "col", "row"),
            P("pipe", None, "col"),
            P("pipe", None, "row"),
            P("pipe", None, "col"),
            P("pipe", None, "row"),
            P(None, "pipe", None, "row"),
            P(None, None, "col"),
            P(),
            P(),
            P(),
            P("col"),
            P(None, "col"),
            P(None, None, "col"),
        ),
        out_specs=(P(None, "pipe", None, "col"), P("pipe", "col", "row")),
        check_vma=False,
    )
```
